128 devices in a mesh: grp: 2 (over x_hi), row: 64 (over y, z, x_lo, core).
Axes of the slice: x: 4 (x_hi: 2, x_lo: 2; x = x_hi * 2 + x_lo), y: 4, z: 4, core: 2. Of those that a mesh axis runs over, the one named last changes fastest.
Arguments:
- saved_rows: float32 [32, 512, 128, 128], P(None, None, ('grp', 'row')), may hold values from -3 to 3
- table_order: int32 [32], replicated, may hold values from 0 to 31, each once
- owner_shard: int32 [32, 128, 128, 1], P(None, ('grp', 'row')), may hold values from 0 to 63; in each aligned block of 128 rows (0 to 127, 128 to 255, ..., all dimensions but the last counted through in order) at most 6 rows name the same one
- row_in_shard: int32 [32, 128, 128], P(None, ('grp', 'row')), may hold values from 0 to 1023
- bag_owner: int32 [32, 128, 128], P(None, ('grp', 'row')), may hold values from 0 to 15, never falling along the last dimension, each value on 1 to 32 neighbouring positions
Outputs:
- pooled: float32 [2048, 32, 128], P(('grp', 'row'))
The draws below stay inside these ranges and needn't reach their ends.
Inputs may be any that keep to these rules, and one draw needn't show every extreme that they name: `owner_shard`: among the 128 ids of one table and one device, no shard number occurs more than 6 times, and 6 is reached in some of these blocks. `bag_owner`: never falls along the last dimension; every sample has 1 to 32 ids of each table. `table_order`: each table number once.
All inputs are finite; a program needn't handle non-finite values.
Results may differ from the reference program's by a relative error of at most 0.00007.
Values sent between devices are 32-bit elements; how exact they have to be, the bound alone decides.
No kernel may reach another device: no remote copies, remote signals or barrier semaphores. Data moves between devices by JAX's collectives and lax.ppermute only.
A program may use at most 128 MiB of HBM per device.

```python
import math
import jax
import jax.numpy as jnp
import numpy as np
from jax import lax

D = 128
TABLES = 32
RS = 512
SAMP_DEV = 16
BAG_MOST = 32
IDS_DEV = 128
RB = 1024
CAP = 6
SAMPLES = 2048
N_ROW = 64
DEVICES = 128


def touch_ends(entries, stream_key, smallest, largest):
    extent = entries.shape
    spot = [jax.random.randint(jax.random.fold_in(stream_key, axis), (), 0, extent[axis]) for axis in range(len(extent))]
    entries = entries.at[tuple(spot)].set(smallest)
    longest = extent.index(max(extent))
    spot[longest] = (spot[longest] + 1) % extent[longest]
    return entries.at[tuple(spot)].set(largest)


def shard_levels(rng, extent, pieces, low, high):
    level = 1.0
    for axis_at, blocks in pieces:
        heights = jax.random.uniform(jax.random.fold_in(jax.random.fold_in(rng, 6), axis_at), (blocks,), jnp.float32, low / len(pieces), high / len(pieces))
        level = level * jnp.repeat(jnp.exp(heights), extent[axis_at] // blocks).reshape((-1,) + (1,) * (len(extent) - 1 - axis_at))
    return level


def rank_table(count, skew):
    loads = [(1 << 20) // math.isqrt(standing ** skew) + 1 for standing in range(1, count + 1)]
    scale = 1 + sum(loads) // (1 << 30)
    return np.cumsum(np.array([max(1, weight // scale) for weight in loads]))


def ranked(rng, extent, number_of, slope):
    table = rank_table(number_of, slope)
    pick = jax.random.randint(jax.random.fold_in(rng, 1), extent, 0, int(table[number_of - 1]))
    standing = jnp.searchsorted(jnp.asarray(table, jnp.int32), pick, side="right")
    return jax.random.permutation(jax.random.fold_in(rng, 2), number_of)[standing].astype(jnp.int32)


def split_up(number_of, total, bound, lean):
    portions = [(1 << 20) // math.isqrt(standing ** lean) + 1 for standing in range(2, number_of + 1)]
    surplus, counts = total - bound - (number_of - 1), [1] * (number_of - 1)
    while surplus > 0:
        free = [i for i in range(number_of - 1) if counts[i] < bound]
        whole, remaining = sum([portions[i] for i in free]), surplus
        for i in free:
            extra = min(bound - counts[i], max(1, remaining * portions[i] // whole), surplus)
            counts[i] = counts[i] + extra
            surplus = surplus - extra
    return np.array([bound] + counts)


def ragged(own_key, amount, total, most, slope):
    if amount == 2:
        one = jax.random.randint(own_key, (), max(1, total - most), min(most, total - 1) + 1)
        return jnp.stack([one, total - one])
    tallies = jnp.asarray(split_up(amount, total, most, slope), jnp.int32)
    couples = (amount - 1) // 2
    donor, receiver = tallies[1:1 + 2 * couples:2], tallies[2:2 + 2 * couples:2]
    margin = jnp.minimum(donor - 1, most - receiver)
    moved = jax.random.randint(jax.random.fold_in(own_key, 1), (couples,), 0, 1 << 20) % (margin + 1)
    tallies = tallies.at[1:1 + 2 * couples:2].set(donor - moved).at[2:2 + 2 * couples:2].set(receiver + moved)
    return tallies[jax.random.permutation(jax.random.fold_in(own_key, 2), amount)]


def assign_block(key, own, number, rows, number_of, top, limit, slope):
    sequence = jax.random.permutation(key, number_of)
    packed, ordinary = load_shares(number_of, rows * top, limit, slope, True), load_shares(number_of, rows * top, limit, slope, False)
    places = jnp.arange(number_of)

    def named(sizes, turn):
        used = int((sizes > 0).sum())
        fixed = max(1, used // 4)
        passed = fixed + (places - fixed + turn * (used - fixed)) % max(1, number_of - fixed)
        return jnp.zeros((number_of,), jnp.int32).at[sequence[jnp.where(places < fixed, places, passed)]].set(jnp.asarray(sizes, jnp.int32))

    sizes = jnp.where(number % 4 == 0, named(packed, number // 4), named(ordinary, number - number // 4 - 1))
    mixed = jax.random.permutation(jax.random.fold_in(own, 3), number_of)
    giver, sink = mixed[0:number_of // 2 * 2:2], mixed[1:number_of // 2 * 2:2]
    margin = jnp.minimum(sizes[giver] - 1, limit - sizes[sink]) // 2
    margin = jnp.where((giver == sequence[0]) | (sink == sequence[0]) | (sizes[sink] == 0), 0, jnp.maximum(margin, 0))
    passed = jax.random.randint(jax.random.fold_in(own, 4), (number_of // 2,), 0, 1 << 20) % (margin + 1)
    sizes = sizes.at[giver].add(-passed).at[sink].add(passed)
    members = jnp.searchsorted(jnp.cumsum(sizes), jnp.arange(rows * top), side="right").astype(jnp.int32)
    table = members.reshape(top, rows).T
    table = table[jax.random.permutation(jax.random.fold_in(own, 1), rows)]
    turn = jax.random.randint(jax.random.fold_in(own, 2), (rows, 1), 0, top)
    return jnp.take_along_axis(table, (jnp.arange(top)[None, :] + turn) % top, axis=1)


def load_shares(number_of, total, most, skew, full):
    weights = [(1 << 20) // math.isqrt(standing ** skew) + 1 for standing in range(1, number_of + 1)]
    largest = most if full else min(most, max(-(-total // number_of), total * weights[0] // sum(weights)))
    least = 1 if total - largest >= number_of - 1 else 0
    given, surplus = [largest] + [least] * (number_of - 1), total - largest - least * (number_of - 1)
    while surplus > 0:
        movable = [i for i in range(1, number_of) if given[i] < largest] or [i for i in range(1, number_of) if given[i] < most]
        pool, left = sum([weights[i] for i in movable]), surplus
        for i in movable:
            addition = min(most - given[i], max(1, left * weights[i] // pool), surplus)
            given[i] = given[i] + addition
            surplus = surplus - addition
    return np.array(given)


def normal_values(own_key, shape, spread, bound, shards=(), kind=jnp.bfloat16):
    drawn = spread * jax.random.normal(own_key, shape, jnp.float32)
    if shards:
        drawn = drawn * shard_levels(own_key, shape, shards, -0.22, 0.18)
    return jnp.clip(drawn, -bound, bound).astype(kind)


def setup_inputs(seed: int = 0) -> dict:
    arg_keys = jax.random.split(jax.random.key(seed), 6)
    saved_rows = normal_values(arg_keys[0], (TABLES, RS, DEVICES, D), 0.5, 3.0, ((2, 128),), jnp.float32)
    table_order = jax.random.permutation(arg_keys[1], TABLES).astype(jnp.int32)
    owner_shard_keys = jax.random.split(jax.random.fold_in(arg_keys[2], 1), TABLES * DEVICES * IDS_DEV // IDS_DEV)
    owner_shard_turns = jax.random.permutation(jax.random.fold_in(arg_keys[2], 3), TABLES * DEVICES * IDS_DEV // IDS_DEV)
    owner_shard = jax.vmap(lambda own, number: assign_block(jax.random.fold_in(arg_keys[2], 2), own, number, IDS_DEV, N_ROW, 1, CAP, 2))(owner_shard_keys, owner_shard_turns).reshape((TABLES, DEVICES, IDS_DEV, 1))
    row_in_shard = touch_ends(ranked(arg_keys[3], (TABLES, DEVICES, IDS_DEV), RB, 2), jax.random.fold_in(arg_keys[3], 3), 0, RB - 1).astype(jnp.int32)
    bag_owner = jax.vmap(lambda own: jnp.searchsorted(jnp.cumsum(ragged(own, SAMP_DEV, IDS_DEV, BAG_MOST, 2)), jnp.arange(IDS_DEV), side="right"))(jax.random.split(arg_keys[4], TABLES * DEVICES)).reshape((TABLES, DEVICES, IDS_DEV)).astype(jnp.int32)
    return dict(saved_rows=saved_rows, table_order=table_order, owner_shard=owner_shard, row_in_shard=row_in_shard, bag_owner=bag_owner)


def pool_table(operands):
    one_table, shard_ids, local_ids, bag_ids = operands
    fetched = one_table[shard_ids * RB + local_ids]
    sample_ids = bag_ids + SAMP_DEV * jnp.arange(DEVICES, dtype=jnp.int32)[:, None]
    return jax.ops.segment_sum(fetched.reshape(-1, D), sample_ids.reshape(-1), num_segments=SAMPLES)


def reference(saved_rows, table_order, owner_shard, row_in_shard, bag_owner):
    tables = saved_rows.reshape(TABLES, RS * DEVICES, D)[table_order]
    per_table = lax.map(pool_table, (tables, owner_shard[table_order][..., 0], row_in_shard[table_order], bag_owner[table_order]))
    return jnp.transpose(per_table, (1, 0, 2))
```

```python
import jax
import jax.numpy as jnp
from jax import lax
from jax.experimental import pallas as pl
from jax.experimental.pallas import tpu as pltpu
from jax.sharding import Mesh, PartitionSpec as P

TABLES = 32
DEPTH = 512
WIDTH = 128
DEVICES = 128
IDS = 128
SAMP = 16
SPAN = 520
ZERO = 516


def place(k):
    return (k >> 6) * 2 + ((k >> 1) & 1), (k >> 4) & 3, (k >> 2) & 3, k & 1


def label(k):
    x, y, z, c = place(k)
    return (((x - z) & 3) * 4 + ((y - z) & 3)) * 2 + c


PLANES = [sorted((k for k in range(DEVICES) if place(k)[2] == z), key=label) for z in range(4)]
HOLDERS = [[PLANES[z][t] for z in range(4)] for t in range(TABLES)]
EVERYONE = [sum(PLANES, [])]


def lookup_kernel(addr, ends, table, out, *sums):
    blocks = len(sums)

    def step(i, carry):
        for j, prefix in enumerate(sums):
            ids = (i * blocks + j) * IDS
            total = jnp.zeros((1, WIDTH), jnp.float32)
            for p in range(IDS):
                total = total + table[pl.ds(addr[ids + p], 1), :]
                prefix[p + 1 : p + 2, :] = total
        for j, prefix in enumerate(sums):
            bag = (i * blocks + j) * SAMP
            below = jnp.zeros((1, WIDTH), jnp.float32)
            for b in range(SAMP):
                upto = prefix[pl.ds(ends[bag + b], 1), :]
                out[pl.ds(bag + b, 1), :] = upto - below
                below = upto
        return carry

    lax.fori_loop(0, DEVICES // blocks, step, 0)


def finish_kernel(order, parts, out):
    for c in range(TABLES):
        t = order[c]
        total = (parts[0, t] + parts[1, t]) + (parts[2, t] + parts[3, t])
        out[:, c, :] = total


def body(saved_rows, table_order, owner_shard, row_in_shard, bag_owner):
    me = lax.axis_index("d")
    x, y, z, c = place(me)
    ids = owner_shard[:, 0, :, 0] * 1024 + row_in_shard[:, 0, :]
    bags = bag_owner[:, 0, :]
    ends = jnp.sum(
        (bags[:, None, :] <= jnp.arange(IDS, dtype=jnp.int32)[None, :, None]).astype(jnp.int32), axis=2
    )
    notes = jnp.stack([ids, ends], axis=1).astype(jnp.float32)
    parcel = jnp.concatenate(
        [
            saved_rows.reshape(TABLES, DEPTH, WIDTH),
            jnp.pad(notes, ((0, 0), (0, SPAN - DEPTH - 2), (0, 0))),
        ],
        axis=1,
    )
    held = lax.all_to_all(parcel, "d", split_axis=0, concat_axis=0, tiled=True, axis_index_groups=PLANES)
    notes = held[:, DEPTH : DEPTH + 2]
    notes = lax.all_gather(notes, "d", axis_index_groups=HOLDERS, axis=0, tiled=True)
    notes = notes.astype(jnp.int32)
    wanted = notes[:, 0, :]
    source = wanted & 127
    addr = label(source) * SPAN + (wanted >> 7)
    addr = jnp.where(place(source)[2] == z, addr, ZERO)
    blocks = 4
    partial = pl.pallas_call(
        lookup_kernel,
        out_shape=jax.ShapeDtypeStruct((DEVICES * SAMP, WIDTH), jnp.float32),
        in_specs=[
            pl.BlockSpec(memory_space=pltpu.SMEM),
            pl.BlockSpec(memory_space=pltpu.SMEM),
            pl.BlockSpec(memory_space=pltpu.VMEM),
        ],
        out_specs=pl.BlockSpec(memory_space=pltpu.VMEM),
        scratch_shapes=[pltpu.VMEM((IDS + 8, WIDTH), jnp.float32)] * blocks,
        compiler_params=pltpu.CompilerParams(vmem_limit_bytes=40 << 20),
        name="lookup",
    )(addr.reshape(-1), notes[:, 1, :SAMP].reshape(-1), held.reshape(TABLES * SPAN, WIDTH))
    parts = lax.all_to_all(
        partial.reshape(DEVICES, SAMP, WIDTH),
        "d",
        split_axis=0,
        concat_axis=0,
        tiled=True,
        axis_index_groups=EVERYONE,
    )
    return pl.pallas_call(
        finish_kernel,
        out_shape=jax.ShapeDtypeStruct((SAMP, TABLES, WIDTH), jnp.float32),
        in_specs=[
            pl.BlockSpec(memory_space=pltpu.SMEM),
            pl.BlockSpec(memory_space=pltpu.VMEM),
        ],
        out_specs=pl.BlockSpec(memory_space=pltpu.VMEM),
        name="finish",
    )(table_order, parts.reshape(4, TABLES, SAMP, WIDTH))


def solution(mesh):
    flat = Mesh(mesh.devices.reshape(DEVICES), ("d",))
    return jax.shard_map(
        body,
        mesh=flat,
        in_specs=(
            P(None, None, "d", None),
            P(),
            P(None, "d", None, None),
            P(None, "d", None),
            P(None, "d", None),
        ),
        out_specs=P("d", None, None),
        check_vma=False,
    )
```

```python
import jax
import jax.numpy as jnp
from jax import lax
from jax.experimental import pallas as pl
from jax.experimental.pallas import tpu as pltpu
from jax.sharding import Mesh, PartitionSpec as P

TABLES = 32
DEPTH = 512
WIDTH = 128
DEVICES = 128
IDS = 128
SAMP = 16
SIZES = (32, 48, 64, 96, 128)
BLOCKS = 4


def place(k):
    return (k >> 6) * 2 + ((k >> 1) & 1), (k >> 4) & 3, (k >> 2) & 3, k & 1


def device(x, y, z, c):
    return (x >> 1) * 64 + y * 16 + z * 4 + (x & 1) * 2 + c


def label(k):
    x, y, z, c = place(k)
    return x * 8 + y * 2 + c


PLANES = [sorted((k for k in range(DEVICES) if place(k)[2] == z), key=label) for z in range(4)]


def moved(axis, by):
    pairs = []
    for k in range(DEVICES):
        at = list(place(k))
        at[axis] = (at[axis] + by) % (2 if axis == 3 else 4)
        pairs.append((k, device(*at)))
    return pairs


def spread(parts, mine, axis, along):
    size = 2 if axis == 3 else 4
    got = []
    for by in range(size):
        piece = lax.dynamic_index_in_dim(parts, (mine + by) & (size - 1), along, keepdims=False)
        got.append(piece if by == 0 else lax.ppermute(piece, "d", moved(axis, by)))
    return jnp.stack(got)


def lookup_kernel(me, addr, ends, table, out, *sums):
    x, y, z, c = place(me[0])

    def step(i, carry):
        first, count = [], []
        for j in range(BLOCKS):
            note = (i * BLOCKS + j) * IDS
            begin = ends[note + z * SAMP]
            first.append(note + begin)
            count.append(ends[note + z * SAMP + SAMP] - begin)
        most = count[0]
        for n in count[1:]:
            most = jnp.maximum(most, n)

        def gather(size):
            for j, prefix in enumerate(sums):
                total = jnp.zeros((1, WIDTH), jnp.float32)
                for p in range(size):
                    total = total + table[pl.ds(addr[first[j] + p], 1), :]
                    prefix[p + 1 : p + 2, :] = total

        below = -1
        for size in SIZES:
            pl.when((most > below) & (most <= size))(lambda size=size: gather(size))
            below = size

        for j, prefix in enumerate(sums):
            b = i * BLOCKS + j
            note = b * IDS + z * SAMP
            begin = ends[note]
            bx = (x - (b & 3)) & 3
            by = (y - ((b >> 2) & 3)) & 3
            bc = c ^ ((b >> 4) & 1)
            bz = (z - ((b >> 5) & 3)) & 3
            row = device(bx, by, bz, bc) * SAMP
            low = jnp.zeros((1, WIDTH), jnp.float32)
            for s in range(SAMP):
                upto = prefix[pl.ds(ends[note + s + 1] - begin, 1), :]
                out[pl.ds(row + s, 1), :] = upto - low
                low = upto
        return carry

    for prefix in sums:
        prefix[0:1, :] = jnp.zeros((1, WIDTH), jnp.float32)
    lax.fori_loop(0, DEVICES // BLOCKS, step, 0)


def finish_kernel(order, parts, out):
    for col in range(TABLES):
        t = order[col]
        x, y, c = t >> 3, (t >> 1) & 3, t & 1
        total = (parts[device(x, y, 0, c)] + parts[device(x, y, 1, c)]) + (
            parts[device(x, y, 2, c)] + parts[device(x, y, 3, c)]
        )
        out[:, col, :] = total


def body(saved_rows, table_order, owner_shard, row_in_shard, bag_owner):
    me = lax.axis_index("d")
    x, y, z, c = place(me)
    held = lax.all_to_all(
        saved_rows.reshape(TABLES, DEPTH, WIDTH),
        "d",
        split_axis=0,
        concat_axis=0,
        tiled=True,
        axis_index_groups=PLANES,
    )

    wanted = owner_shard[:, 0, :, 0] * 1024 + row_in_shard[:, 0, :]
    bags = bag_owner[:, 0, :]
    source = wanted & 127
    sx, sy, plane, sc = place(source)
    addr = (sx * 8 + sy * 2 + sc) * DEPTH + (wanted >> 7)
    lanes = jnp.arange(IDS, dtype=jnp.int32)
    is_in = (plane[:, None, :] == jnp.arange(4, dtype=jnp.int32)[None, :, None]).astype(jnp.float32)
    upto = (lanes[:, None] <= lanes[None, :]).astype(jnp.float32)
    rank = jnp.einsum("tzp,pq->tzq", is_in, upto)
    amount = rank[:, :, IDS - 1]
    offset = jnp.cumsum(amount, axis=1) - amount
    slot = jnp.sum(is_in * (rank + offset[:, :, None] - 1.0), axis=1).astype(jnp.int32)
    order = jnp.sum(
        jnp.where(slot[:, None, :] == lanes[None, :, None], addr[:, None, :], 0), axis=2
    )
    below = (bags[:, None, :] <= jnp.arange(SAMP, dtype=jnp.int32)[None, :, None]).astype(jnp.float32)
    ends = jnp.einsum("tzp,tbp->tzb", is_in, below) + offset[:, :, None]
    ends = jnp.pad(ends.reshape(TABLES, 4 * SAMP), ((0, 0), (1, IDS - 1 - 4 * SAMP)))
    notes = jnp.stack([order.astype(jnp.float32), ends], axis=1)

    notes = spread(notes.reshape(4, 4, 2, 2, IDS), x, 0, 0)
    notes = spread(notes, y, 1, 1)
    notes = spread(notes, c, 3, 2)
    notes = jnp.stack([notes] + [lax.ppermute(notes, "d", moved(2, by)) for by in (1, 2, 3)])
    notes = notes.reshape(DEVICES, 2, IDS).astype(jnp.int32)
    addr = jnp.pad(notes[:, 0].reshape(-1), (0, IDS))
    ends = notes[:, 1].reshape(-1)

    partial = pl.pallas_call(
        lookup_kernel,
        out_shape=jax.ShapeDtypeStruct((DEVICES * SAMP, WIDTH), jnp.float32),
        in_specs=[
            pl.BlockSpec(memory_space=pltpu.SMEM),
            pl.BlockSpec(memory_space=pltpu.SMEM),
            pl.BlockSpec(memory_space=pltpu.SMEM),
            pl.BlockSpec(memory_space=pltpu.VMEM),
        ],
        out_specs=pl.BlockSpec(memory_space=pltpu.VMEM),
        scratch_shapes=[pltpu.VMEM((IDS + 8, WIDTH), jnp.float32)] * BLOCKS,
        compiler_params=pltpu.CompilerParams(vmem_limit_bytes=40 << 20),
        name="lookup",
    )(me.reshape(1), addr, ends, held.reshape(TABLES * DEPTH, WIDTH))
    parts = lax.all_to_all(
        partial.reshape(DEVICES, SAMP, WIDTH), "d", split_axis=0, concat_axis=0, tiled=True
    )
    return pl.pallas_call(
        finish_kernel,
        out_shape=jax.ShapeDtypeStruct((SAMP, TABLES, WIDTH), jnp.float32),
        in_specs=[
            pl.BlockSpec(memory_space=pltpu.SMEM),
            pl.BlockSpec(memory_space=pltpu.VMEM),
        ],
        out_specs=pl.BlockSpec(memory_space=pltpu.VMEM),
        name="finish",
    )(table_order, parts)


def solution(mesh):
    flat = Mesh(mesh.devices.reshape(DEVICES), ("d",))
    return jax.shard_map(
        body,
        mesh=flat,
        in_specs=(
            P(None, None, "d", None),
            P(),
            P(None, "d", None, None),
            P(None, "d", None),
            P(None, "d", None),
        ),
        out_specs=P("d", None, None),
        check_vma=False,
    )
```

```python
import functools

import jax
import jax.numpy as jnp
from jax import lax
from jax.experimental import pallas as pl
from jax.experimental.pallas import tpu as pltpu
from jax.sharding import Mesh, PartitionSpec as P


TABLES = 32
DEPTH = 512
WIDTH = 128
DEVICES = 128
IDS = 128
SAMP = 16
SIZES = (32, 48, 64, 96, 128)
BLOCKS = 4
STARTS = (0, 160, 336)
DATA = (160, 176, 176)
ROWS = (168, 176, 176)
BASES = (0, 32 * 168, 32 * (168 + 176))
HELD = 32 * (168 + 176 + 176)
FIRST_AXIS = (1, 2, 0)
SECOND_AXIS = (0, 1, 2)


def place(k):
    return (k >> 6) * 2 + ((k >> 1) & 1), (k >> 4) & 3, (k >> 2) & 3, k & 1


def device(x, y, z, c):
    return (x >> 1) * 64 + y * 16 + z * 4 + (x & 1) * 2 + c


def moved(axis, by):
    pairs = []
    for k in range(DEVICES):
        at = list(place(k))
        at[axis] = (at[axis] + by) % (2 if axis == 3 else 4)
        pairs.append((k, device(*at)))
    return pairs


def in_vmem(count):
    return [pl.BlockSpec(memory_space=pltpu.VMEM)] * count


SCALARS = pl.BlockSpec(memory_space=pltpu.SMEM)


def first_kernel(way, me, own, other, *outs):
    x, y, z, c = place(me[0])
    for by in range(4):
        for j in range(4):
            if way == 0:
                t = j * 4 + ((y + by - z) & 3)
            elif way == 1:
                t = ((x - z - by) & 3) * 4 + j
            else:
                t = ((j + x + by - y) & 3) * 4 + j
            outs[by][0, j] = own[t]
            outs[by][1, j] = other[t]


def second_kernel(way, me, *refs):
    gots, outs = refs[:4], refs[4:]
    x, y, z, c = place(me[0])
    for by in range(4):
        if way == 0:
            j = (x + by - z) & 3
        elif way == 1:
            j = (y + by - z) & 3
        else:
            j = (y - z - by) & 3
        for step in range(4):
            for core in range(2):
                outs[by][step, core] = gots[step][core, j]


def restore(me, saved, notes):
    c = me[0] & 1
    pieces = []
    for way in range(3):

        def half(core, way=way):
            rows = lax.dynamic_slice(saved, (0, core, STARTS[way], 0), (16, 1, DATA[way], WIDTH))[:, 0]
            if way:
                return rows
            return jnp.concatenate([rows, lax.dynamic_index_in_dim(notes, core, 1, keepdims=False)], axis=1)

        other = lax.ppermute(half(1 - c), "d", moved(3, 1))
        sent = pl.pallas_call(
            functools.partial(first_kernel, way),
            out_shape=[jax.ShapeDtypeStruct((2, 4, ROWS[way], WIDTH), jnp.float32)] * 4,
            in_specs=[SCALARS] + in_vmem(2),
            out_specs=in_vmem(4),
            compiler_params=pltpu.CompilerParams(vmem_limit_bytes=10 << 20),
            name=f"first{way}",
        )(me, half(c), other)
        got = [sent[0]] + [lax.ppermute(sent[by], "d", moved(FIRST_AXIS[way], by)) for by in (1, 2, 3)]
        sent = pl.pallas_call(
            functools.partial(second_kernel, way),
            out_shape=[jax.ShapeDtypeStruct((4, 2, ROWS[way], WIDTH), jnp.float32)] * 4,
            in_specs=[SCALARS] + in_vmem(4),
            out_specs=in_vmem(4),
            compiler_params=pltpu.CompilerParams(vmem_limit_bytes=10 << 20),
            name=f"second{way}",
        )(me, *got)
        pieces += [sent[0]] + [lax.ppermute(sent[by], "d", moved(SECOND_AXIS[way], by)) for by in (1, 2, 3)]
    return pieces


def lookup_kernel(me, *refs):
    pieces, out, table, words, notes, sem = refs[:12], refs[12], refs[13], refs[14], refs[15], refs[16]
    sums = refs[17:]
    x, y, z, c = place(me[0])
    for xs in range(4):
        for ys in range(4):
            for core in range(2):
                at = (xs * 4 + ys) * 2 + core
                both = pieces[xs][ys, core, DATA[0] :, :].astype(jnp.int32)
                words[at * 4 : at * 4 + 4, :IDS] = both[:4]
                words[at * 4 : at * 4 + 4, IDS:] = both[4:]
    fetch = pltpu.make_async_copy(words, notes, sem)
    fetch.start()
    for way in range(3):
        for by in range(4):
            piece = pieces[way * 4 + by]

            def put(i, carry, piece=piece, way=way, by=by):
                to = pl.multiple_of(BASES[way] + by * 8 * ROWS[way] + i * ROWS[way], 8)
                table[pl.ds(to, ROWS[way]), :] = piece[i >> 1, i & 1]
                return carry

            lax.fori_loop(0, 8, put, 0)
    fetch.wait()

    def step(i, carry):
        first, count = [], []
        for j in range(BLOCKS):
            note = i * BLOCKS + j
            begin = notes[note, IDS + z * SAMP]
            first.append((note, begin))
            count.append(notes[note, IDS + z * SAMP + SAMP] - begin)
        most = count[0]
        for n in count[1:]:
            most = jnp.maximum(most, n)

        def gather(size):
            for j, prefix in enumerate(sums):
                note, begin = first[j]
                total = jnp.zeros((1, WIDTH), jnp.float32)
                for p in range(size):
                    total = total + table[pl.ds(notes[note, begin + p], 1), :]
                    prefix[p + 1 : p + 2, :] = total

        below = -1
        for size in SIZES:
            pl.when((most > below) & (most <= size))(lambda size=size: gather(size))
            below = size

        for j, prefix in enumerate(sums):
            note, begin = first[j]
            bx = (x - (note >> 5)) & 3
            by = (y - ((note >> 3) & 3)) & 3
            bc = c ^ ((note >> 2) & 1)
            bz = (z - (note & 3)) & 3
            row = device(bx, by, bz, bc) * SAMP
            low = jnp.zeros((1, WIDTH), jnp.float32)
            for s in range(SAMP):
                upto = prefix[pl.ds(notes[note, IDS + z * SAMP + s + 1] - begin, 1), :]
                out[pl.ds(row + s, 1), :] = upto - low
                low = upto
        return carry

    for prefix in sums:
        prefix[0:1, :] = jnp.zeros((1, WIDTH), jnp.float32)
    lax.fori_loop(0, DEVICES // BLOCKS, step, 0)


def finish_kernel(order, parts, out):
    for col in range(TABLES):
        t = order[col]
        a, b, c = t >> 3, (t >> 1) & 3, t & 1
        at = [device((a + z) & 3, (b + z) & 3, z, c) for z in range(4)]
        out[:, col, :] = (parts[at[0]] + parts[at[1]]) + (parts[at[2]] + parts[at[3]])


def body(saved_rows, table_order, owner_shard, row_in_shard, bag_owner):
    me = lax.axis_index("d")
    wanted = owner_shard[:, 0, :, 0] * 1024 + row_in_shard[:, 0, :]
    bags = bag_owner[:, 0, :]
    depth = wanted >> 7
    sx, sy, sz, sc = place(wanted & 127)
    tables = jnp.arange(TABLES, dtype=jnp.int32)[:, None]
    a, b, c = tables >> 3, (tables >> 1) & 3, tables & 1
    ways = [depth < STARTS[1], (depth >= STARTS[1]) & (depth < STARTS[2]), depth >= STARTS[2]]
    holder = jnp.where(ways[0], sz, jnp.where(ways[1], (sx - a) & 3, (sy - b) & 3))
    back = ((a + holder - sx) & 3, (b + holder - sy) & 3, (holder - sz) & 3)
    addr = 0
    for way in range(3):
        at = (back[SECOND_AXIS[way]] * 4 + back[FIRST_AXIS[way]]) * 2 + (c ^ sc)
        at = at * ROWS[way] + (BASES[way] - STARTS[way]) + depth
        addr = addr + jnp.where(ways[way], at, 0)

    lanes = jnp.arange(IDS, dtype=jnp.int32)
    is_in = (holder[:, None, :] == jnp.arange(4, dtype=jnp.int32)[None, :, None]).astype(jnp.float32)
    upto = (lanes[:, None] <= lanes[None, :]).astype(jnp.float32)
    rank = jnp.einsum("tzp,pq->tzq", is_in, upto)
    amount = rank[:, :, IDS - 1]
    offset = jnp.cumsum(amount, axis=1) - amount
    slot = jnp.sum(is_in * (rank + offset[:, :, None] - 1.0), axis=1).astype(jnp.int32)
    order = jnp.sum(jnp.where(slot[:, None, :] == lanes[None, :, None], addr[:, None, :], 0), axis=2)
    below = (bags[:, None, :] <= jnp.arange(SAMP, dtype=jnp.int32)[None, :, None]).astype(jnp.float32)
    ends = jnp.einsum("tzp,tbp->tzb", is_in, below) + offset[:, :, None]
    ends = jnp.pad(ends.reshape(TABLES, 4 * SAMP), ((0, 0), (1, IDS - 1 - 4 * SAMP)))
    notes = jnp.stack([order.astype(jnp.float32), ends], axis=1)
    notes = [notes] + [lax.ppermute(notes, "d", moved(2, by)) for by in (1, 2, 3)]
    notes = jnp.concatenate([n[:, :1] for n in notes] + [n[:, 1:] for n in notes], axis=1)

    scalars = me.reshape(1)
    pieces = restore(
        scalars, saved_rows.reshape(16, 2, DEPTH, WIDTH), notes.reshape(16, 2, 8, WIDTH)
    )
    partial = pl.pallas_call(
        lookup_kernel,
        out_shape=jax.ShapeDtypeStruct((DEVICES * SAMP, WIDTH), jnp.float32),
        in_specs=[SCALARS] + in_vmem(12),
        out_specs=in_vmem(1)[0],
        scratch_shapes=[
            pltpu.VMEM((HELD, WIDTH), jnp.float32),
            pltpu.VMEM((DEVICES, 2 * IDS), jnp.int32),
            pltpu.SMEM((DEVICES, 2 * IDS), jnp.int32),
            pltpu.SemaphoreType.DMA,
        ]
        + [pltpu.VMEM((IDS + 8, WIDTH), jnp.float32)] * BLOCKS,
        compiler_params=pltpu.CompilerParams(vmem_limit_bytes=30 << 20),
        name="lookup",
    )(scalars, *pieces)
    parts = lax.all_to_all(
        partial.reshape(DEVICES, SAMP, WIDTH), "d", split_axis=0, concat_axis=0, tiled=True
    )
    return pl.pallas_call(
        finish_kernel,
        out_shape=jax.ShapeDtypeStruct((SAMP, TABLES, WIDTH), jnp.float32),
        in_specs=[SCALARS] + in_vmem(1),
        out_specs=in_vmem(1)[0],
        name="finish",
    )(table_order, parts)


def solution(mesh):
    flat = Mesh(mesh.devices.reshape(DEVICES), ("d",))
    return jax.shard_map(
        body,
        mesh=flat,
        in_specs=(
            P(None, None, "d", None),
            P(),
            P(None, "d", None, None),
            P(None, "d", None),
            P(None, "d", None),
        ),
        out_specs=P("d", None, None),
        check_vma=False,
    )
```

```python
import functools

import jax
import jax.numpy as jnp
from jax import lax
from jax.experimental import pallas as pl
from jax.experimental.pallas import tpu as pltpu
from jax.sharding import Mesh, PartitionSpec as P


TABLES = 32
DEPTH = 512
WIDTH = 128
DEVICES = 128
IDS = 128
SAMP = 16
BLOCKS = 8
CHUNK = 8
STARTS = (0, 160, 336)
DATA = (160, 176, 176)
ROWS = (168, 176, 176)
BASES = (0, 32 * 168, 32 * (168 + 176))
HELD = 32 * (168 + 176 + 176)
FIRST_AXIS = (1, 2, 0)
SECOND_AXIS = (0, 1, 2)


def place(k):
    return (k >> 6) * 2 + ((k >> 1) & 1), (k >> 4) & 3, (k >> 2) & 3, k & 1


def device(x, y, z, c):
    return (x >> 1) * 64 + y * 16 + z * 4 + (x & 1) * 2 + c


def moved(axis, by):
    pairs = []
    for k in range(DEVICES):
        at = list(place(k))
        at[axis] = (at[axis] + by) % (2 if axis == 3 else 4)
        pairs.append((k, device(*at)))
    return pairs


def in_vmem(count):
    return [pl.BlockSpec(memory_space=pltpu.VMEM)] * count


SCALARS = pl.BlockSpec(memory_space=pltpu.SMEM)


def send(value, axis, by):
    return lax.ppermute(value, "d", moved(axis, by))


def half_kernel(theirs, me, saved, out0, out1, out2, sems):
    c = me[0] & 1
    core = 1 - c if theirs else c
    copies = [
        pltpu.make_async_copy(
            saved.at[:, core, pl.ds(STARTS[way], DATA[way]), :], out, sems.at[way]
        )
        for way, out in enumerate((out0, out1, out2))
    ]
    for copy in copies:
        copy.start()
    for copy in copies:
        copy.wait()


def attach_kernel(me, rows, notes, out):
    out[:, : DATA[0], :] = rows[...]
    out[:, DATA[0] :, :] = notes[...]


def first_kernel(way, me, own, other, *refs):
    notes, outs = refs[:-4], refs[-4:]
    x, y, z, _ = place(me[0])
    for by in range(4):
        for j in range(4):
            if way == 0:
                t = j * 4 + ((y + by - z) & 3)
            elif way == 1:
                t = ((x - z - by) & 3) * 4 + j
            else:
                t = ((j + x + by - y) & 3) * 4 + j
            outs[by][0, j, : DATA[way], :] = own[t]
            outs[by][1, j] = other[t]
            if notes:
                outs[by][0, j, DATA[way] :, :] = notes[0][t]


def second_kernel(way, me, *refs):
    gots, outs = refs[:4], refs[4:]
    x, y, z, _ = place(me[0])
    for by in range(4):
        if way == 0:
            j = (x + by - z) & 3
        elif way == 1:
            j = (y + by - z) & 3
        else:
            j = (y - z - by) & 3
        for step in range(4):
            for core in range(2):
                outs[by][step, core] = gots[step][core, j]


def notes_kernel(me, owner, row, bag, out):
    c = me[0] & 1
    wanted = owner[...] * 1024 + row[...]
    depth = wanted >> 7
    sx, sy, sz, sc = place(wanted & 127)
    table = lax.broadcasted_iota(jnp.int32, (TABLES, IDS), 0)
    ta, tb, tc = table >> 3, (table >> 1) & 3, table & 1
    ways = [depth < STARTS[1], (depth >= STARTS[1]) & (depth < STARTS[2]), depth >= STARTS[2]]
    holder = jnp.where(ways[0], sz, jnp.where(ways[1], (sx - ta) & 3, (sy - tb) & 3))
    back = ((ta + holder - sx) & 3, (tb + holder - sy) & 3, (holder - sz) & 3)
    addr = jnp.zeros((TABLES, IDS), jnp.int32)
    for way in range(3):
        at = (back[SECOND_AXIS[way]] * 4 + back[FIRST_AXIS[way]]) * 2 + (tc ^ sc)
        addr = jnp.where(ways[way], at * ROWS[way] + (BASES[way] - STARTS[way]) + depth, addr)

    upper = lax.broadcasted_iota(jnp.int32, (IDS, IDS), 0) <= lax.broadcasted_iota(jnp.int32, (IDS, IDS), 1)
    upper = upper.astype(jnp.float32)
    is_in = [(holder == z).astype(jnp.float32) for z in range(4)]
    slot = jnp.zeros((TABLES, IDS), jnp.float32)
    offset = jnp.zeros((TABLES, 1), jnp.float32)
    for z in range(4):
        rank = jnp.dot(is_in[z], upper, preferred_element_type=jnp.float32)
        slot = slot + is_in[z] * (rank + (offset - 1.0))
        offset = offset + jnp.sum(is_in[z], axis=1, keepdims=True)
    slots = jnp.transpose(slot)
    bags = jnp.transpose(bag[...].astype(jnp.float32))
    high, low = (addr >> 8).astype(jnp.float32), (addr & 255).astype(jnp.float32)

    lane = lax.broadcasted_iota(jnp.int32, (IDS, IDS), 1)
    lanes = lane.astype(jnp.float32)
    bound = jnp.where((lane & 31) == 0, SAMP, (lane & 31) - 1).astype(jnp.float32)
    kind = lax.broadcasted_iota(jnp.int32, (8, IDS), 0) - 2
    at = lax.broadcasted_iota(jnp.int32, (8, IDS), 1)
    before = ((at & 31) == 0) & (kind < (at >> 5)) & (kind >= 0)
    counted = (before | (((at & 31) != 0) & (kind == (at >> 5)))).astype(jnp.float32)
    for ab in range(16):
        both = []
        for t in (2 * ab, 2 * ab + 1):
            rows = [high[t : t + 1], low[t : t + 1]] + [m[t : t + 1] for m in is_in]
            rows = jnp.concatenate(rows + [jnp.zeros((2, IDS), jnp.float32)], axis=0)
            chosen = (slots[:, t : t + 1] == lanes).astype(jnp.float32)
            within = (bags[:, t : t + 1] <= bound).astype(jnp.float32)
            got = jnp.dot(rows, chosen, preferred_element_type=jnp.float32)
            ends = jnp.dot(rows, within, preferred_element_type=jnp.float32)
            both.append((got[0:1] * 256.0 + got[1:2], jnp.sum(ends * counted, axis=0, keepdims=True)))
        for part, first in enumerate((0, 16)):
            out[0, first + ab : first + ab + 1, :] = jnp.where(c == 0, both[0][part], both[1][part])
            out[1, first + ab : first + ab + 1, :] = jnp.where(c == 0, both[1][part], both[0][part])


def gather_kernel(me, *refs):
    for ab in range(16):
        for step in range(4):
            for part in range(2):
                for half in range(2):
                    line = refs[step][half, part * 16 + ab : part * 16 + ab + 1, :]
                    refs[4 + half][ab, part * 4 + step : part * 4 + step + 1, :] = line


def pack(kernel, shapes, me, *args):
    return list(pl.pallas_call(
        kernel,
        out_shape=[jax.ShapeDtypeStruct(shape + (WIDTH,), jnp.float32) for shape in shapes],
        in_specs=[SCALARS] + in_vmem(len(args)),
        out_specs=in_vmem(len(shapes)),
        compiler_params=pltpu.CompilerParams(vmem_limit_bytes=6 << 20),
    )(me, *args))


def halves(me, saved, theirs):
    return list(pl.pallas_call(
        functools.partial(half_kernel, theirs),
        out_shape=[jax.ShapeDtypeStruct((16, DATA[way], WIDTH), jnp.float32) for way in range(3)],
        in_specs=[SCALARS, pl.BlockSpec(memory_space=pltpu.HBM)],
        out_specs=in_vmem(3),
        scratch_shapes=[pltpu.SemaphoreType.DMA((3,))],
        compiler_params=pltpu.CompilerParams(vmem_limit_bytes=46 << 20),
    )(me, saved))


def restore(me, saved, lists):
    theirs = halves(me, saved, True)
    (notes,) = pack(notes_kernel, [(2, TABLES)], me, *lists)
    own = halves(me, saved, False)
    notes = [notes] + [send(notes, 2, by) for by in (1, 2, 3)]
    notes = pack(gather_kernel, [(16, 8)] * 2, me, *notes)
    (theirs[0],) = pack(attach_kernel, [(16, ROWS[0])], me, theirs[0], notes[1])
    pieces = []
    for way in range(3):
        extra = [notes[0]] if way == 0 else []
        other = send(theirs[way], 3, 1)
        shapes = [(2, 4, ROWS[way])] * 4
        kernel = functools.partial(first_kernel, way)
        sent = pack(kernel, shapes, me, own[way], other, *extra)
        got = [sent[0]] + [send(sent[by], FIRST_AXIS[way], by) for by in (1, 2, 3)]
        shapes = [(4, 2, ROWS[way])] * 4
        sent = pack(functools.partial(second_kernel, way), shapes, me, *got)
        pieces += [sent[0]] + [send(sent[by], SECOND_AXIS[way], by) for by in (1, 2, 3)]
    return pieces


def lookup_kernel(me, addr, ends, *refs):
    pieces, out, table, sums = refs[:12], refs[12], refs[13], refs[14:]
    x, y, z, c = place(me[0])
    for way in range(3):
        for by in range(4):
            piece = pieces[way * 4 + by]

            def put(i, carry, piece=piece, way=way, by=by):
                to = pl.multiple_of(BASES[way] + by * 8 * ROWS[way] + i * ROWS[way], 8)
                table[pl.ds(to, ROWS[way]), :] = piece[i >> 1, i & 1]
                return carry

            lax.fori_loop(0, 8, put, 0)

    def step(i, carry):
        note = [(i * BLOCKS + j) * IDS for j in range(BLOCKS)]
        info = [n + z * 32 for n in note]
        first = [note[j] + ends[info[j]] for j in range(BLOCKS)]
        most = ends[info[0] + SAMP]
        for j in range(1, BLOCKS):
            most = jnp.maximum(most, ends[info[j] + SAMP])

        def chunk(k, totals):
            totals = list(totals)
            at = [f + k * CHUNK for f in first]
            to = k * CHUNK + 1
            for p in range(CHUNK):
                for j, prefix in enumerate(sums):
                    totals[j] = totals[j] + table[pl.ds(addr[at[j] + p], 1), :]
                    prefix[pl.ds(to + p, 1), :] = totals[j]
            return tuple(totals)

        lax.fori_loop(0, (most + CHUNK - 1) // CHUNK, chunk, (jnp.zeros((1, WIDTH), jnp.float32),) * BLOCKS)

        for j, prefix in enumerate(sums):
            b = i * BLOCKS + j
            bx = (x - (b >> 5)) & 3
            by = (y - ((b >> 3) & 3)) & 3
            bc = c ^ ((b >> 2) & 1)
            bz = (z - (b & 3)) & 3
            row = device(bx, by, bz, bc) * SAMP
            low = jnp.zeros((1, WIDTH), jnp.float32)
            for s in range(SAMP):
                upto = prefix[pl.ds(ends[info[j] + s + 1], 1), :]
                out[pl.ds(row + s, 1), :] = upto - low
                low = upto
        return carry

    for prefix in sums:
        prefix[0:1, :] = jnp.zeros((1, WIDTH), jnp.float32)
    lax.fori_loop(0, DEVICES // BLOCKS, step, 0)


def finish_kernel(order, parts, out):
    for col in range(TABLES):
        t = order[col]
        a, b, c = t >> 3, (t >> 1) & 3, t & 1
        at = [device((a + z) & 3, (b + z) & 3, z, c) for z in range(4)]
        out[:, col, :] = (parts[at[0]] + parts[at[1]]) + (parts[at[2]] + parts[at[3]])


def program(saved_rows, table_order, owner_shard, row_in_shard, bag_owner):
    me = lax.axis_index("d")
    scalars = me.reshape(1)
    lists = (owner_shard.reshape(TABLES, IDS), row_in_shard.reshape(TABLES, IDS), bag_owner.reshape(TABLES, IDS))
    pieces = restore(scalars, saved_rows.reshape(16, 2, DEPTH, WIDTH), lists)
    notes = jnp.stack([piece[:, :, DATA[0] :, :] for piece in pieces[:4]])
    notes = notes.reshape(DEVICES // 4, 2, 4, IDS).astype(jnp.int32)
    addr = jnp.pad(notes[:, 0].reshape(-1), (0, 2 * IDS))
    ends = notes[:, 1].reshape(-1)
    partial = pl.pallas_call(
        lookup_kernel,
        out_shape=jax.ShapeDtypeStruct((DEVICES * SAMP, WIDTH), jnp.float32),
        in_specs=[SCALARS] * 3 + in_vmem(12),
        out_specs=in_vmem(1)[0],
        scratch_shapes=[pltpu.VMEM((HELD, WIDTH), jnp.float32)]
        + [pltpu.VMEM((IDS + 8, WIDTH), jnp.float32)] * BLOCKS,
        compiler_params=pltpu.CompilerParams(vmem_limit_bytes=12 << 20),
        name="lookup",
    )(scalars, addr, ends, *pieces)
    parts = lax.all_to_all(
        partial.reshape(DEVICES, SAMP, WIDTH), "d", split_axis=0, concat_axis=0, tiled=True
    )
    return pl.pallas_call(
        finish_kernel,
        out_shape=jax.ShapeDtypeStruct((SAMP, TABLES, WIDTH), jnp.float32),
        in_specs=[SCALARS] + in_vmem(1),
        out_specs=in_vmem(1)[0],
        name="finish",
    )(table_order, parts)


def solution(mesh):
    flat = Mesh(mesh.devices.reshape(DEVICES), ("d",))
    return jax.shard_map(
        program,
        mesh=flat,
        in_specs=(
            P(None, None, "d", None),
            P(),
            P(None, "d", None, None),
            P(None, "d", None),
            P(None, "d", None),
        ),
        out_specs=P("d", None, None),
        check_vma=False,
    )
```

```python
import functools

import jax
import jax.numpy as jnp
from jax import lax
from jax.experimental import pallas as pl
from jax.experimental.pallas import tpu as pltpu
from jax.sharding import Mesh, PartitionSpec as P


TABLES = 32
DEPTH = 512
WIDTH = 128
DEVICES = 128
IDS = 128
SAMP = 16
BLOCKS = 8
CHUNK = 8
NEAREST = {
    (1, 0): (1, 0, 0),
    (3, 0): (-1, 0, 0),
    (0, 1): (0, 1, 0),
    (0, 3): (0, -1, 0),
    (1, 1): (0, 0, -1),
    (3, 3): (0, 0, 1),
    (2, 0): (2, 0, 0),
    (0, 2): (0, 2, 0),
    (2, 2): (0, 0, 2),
    (2, 1): (1, 0, -1),
    (3, 2): (0, -1, 1),
    (3, 1): (-1, 1, 0),
    (2, 3): (-1, 0, 1),
    (1, 2): (0, 1, -1),
    (1, 3): (1, -1, 0),
    (0, 0): (0, 0, 0),
}
CLASSES = list(NEAREST)


def place(k):
    return (k >> 6) * 2 + ((k >> 1) & 1), (k >> 4) & 3, (k >> 2) & 3, k & 1


def device(x, y, z, c):
    return (x >> 1) * 64 + y * 16 + z * 4 + (x & 1) * 2 + c


def moved(step):
    pairs = []
    for k in range(DEVICES):
        at = [p + d for p, d in zip(place(k), step)]
        pairs.append((k, device(*[p & 3 for p in at[:3]], at[3] & 1)))
    return pairs


def holders(t):
    a, b, c = t >> 3, (t >> 1) & 3, t & 1
    return [device((a + z) & 3, (b + z) & 3, z, c) for z in range(4)]


def in_vmem(count):
    return [pl.BlockSpec(memory_space=pltpu.VMEM)] * count


SCALARS = pl.BlockSpec(memory_space=pltpu.SMEM)


def send(value, step):
    return lax.ppermute(value, "d", moved(step))


def half_kernel(theirs, me, saved, *refs):
    outs, sems = refs[:-1], refs[-1]
    x, y, z, c = place(me[0])
    core = 1 - c if theirs else c
    copies = []
    for n, (u, v) in enumerate(CLASSES):
        t = ((x - z - u) & 3) * 4 + ((y - z - v) & 3)
        to = outs[n // 4].at[n % 4] if theirs else outs[0].at[n]
        copies.append(pltpu.make_async_copy(saved.at[t, core], to, sems.at[n]))
        copies[-1].start()
    for copy in copies:
        copy.wait()


def pack_kernel(first, me, own, other, *outs):
    for n, out in enumerate(outs):
        out[0] = own[first + n]
        out[1] = other[n]


def notes_kernel(me, owner, row, bag, out):
    wanted = owner[...] * 1024 + row[...]
    depth = wanted >> 7
    sx, sy, sz, sc = place(wanted & 127)
    table = lax.broadcasted_iota(jnp.int32, (TABLES, IDS), 0)
    ta, tb, tc = table >> 3, (table >> 1) & 3, table & 1
    u, v = (sx - sz - ta) & 3, (sy - sz - tb) & 3
    kind = u * 4 + v
    holder = jnp.zeros((TABLES, IDS), jnp.int32)
    for (cu, cv), step in NEAREST.items():
        holder = jnp.where(kind == cu * 4 + cv, step[2], holder)
    holder = (sz - holder) & 3
    addr = (kind * 2 + (tc ^ sc)) * DEPTH + depth

    upper = lax.broadcasted_iota(jnp.int32, (IDS, IDS), 0) <= lax.broadcasted_iota(jnp.int32, (IDS, IDS), 1)
    upper = upper.astype(jnp.float32)
    is_in = [(holder == z).astype(jnp.float32) for z in range(4)]
    slot = jnp.zeros((TABLES, IDS), jnp.float32)
    offset = jnp.zeros((TABLES, 1), jnp.float32)
    for z in range(4):
        rank = jnp.dot(is_in[z], upper, preferred_element_type=jnp.float32)
        slot = slot + is_in[z] * (rank + (offset - 1.0))
        offset = offset + jnp.sum(is_in[z], axis=1, keepdims=True)
    slots = jnp.transpose(slot)
    bags = jnp.transpose(bag[...].astype(jnp.float32))
    high, low = (addr >> 8).astype(jnp.float32), (addr & 255).astype(jnp.float32)

    lane = lax.broadcasted_iota(jnp.int32, (IDS, IDS), 1)
    lanes = lane.astype(jnp.float32)
    bound = jnp.where((lane & 31) == 0, SAMP, (lane & 31) - 1).astype(jnp.float32)
    kind = lax.broadcasted_iota(jnp.int32, (8, IDS), 0) - 2
    at = lax.broadcasted_iota(jnp.int32, (8, IDS), 1)
    before = ((at & 31) == 0) & (kind < (at >> 5)) & (kind >= 0)
    counted = (before | (((at & 31) != 0) & (kind == (at >> 5)))).astype(jnp.float32)
    for t in range(TABLES):
        rows = [high[t : t + 1], low[t : t + 1]] + [m[t : t + 1] for m in is_in]
        rows = jnp.concatenate(rows + [jnp.zeros((2, IDS), jnp.float32)], axis=0)
        chosen = (slots[:, t : t + 1] == lanes).astype(jnp.float32)
        within = (bags[:, t : t + 1] <= bound).astype(jnp.float32)
        got = jnp.dot(rows, chosen, preferred_element_type=jnp.float32)
        ends = jnp.dot(rows, within, preferred_element_type=jnp.float32)
        got = got[0:1] * 256.0 + got[1:2]
        ends = jnp.sum(ends * counted, axis=0, keepdims=True)
        for k in holders(t):
            out[k, 0:1, :] = got
            out[k, 1:2, :] = ends


def pack(kernel, shapes, me, *args):
    return list(pl.pallas_call(
        kernel,
        out_shape=[jax.ShapeDtypeStruct(shape + (WIDTH,), jnp.float32) for shape in shapes],
        in_specs=[SCALARS] + in_vmem(len(args)),
        out_specs=in_vmem(len(shapes)),
        compiler_params=pltpu.CompilerParams(vmem_limit_bytes=6 << 20),
    )(me, *args))


def halves(theirs, shapes, me, saved):
    return list(pl.pallas_call(
        functools.partial(half_kernel, theirs),
        out_shape=[jax.ShapeDtypeStruct(shape + (WIDTH,), jnp.float32) for shape in shapes],
        in_specs=[SCALARS, pl.BlockSpec(memory_space=pltpu.HBM)],
        out_specs=in_vmem(len(shapes)),
        scratch_shapes=[pltpu.SemaphoreType.DMA((16,))],
        compiler_params=pltpu.CompilerParams(vmem_limit_bytes=46 << 20),
    )(me, saved))


def restore(me, saved):
    theirs = halves(True, [(4, DEPTH)] * 4, me, saved)
    others = [send(theirs[m], (0, 0, 0, 1)) for m in range(4)]
    (own,) = halves(False, [(16, DEPTH)], me, saved)
    pieces = {}
    for m in range(4):
        kernel = functools.partial(pack_kernel, 4 * m)
        parts = pack(kernel, [(2, DEPTH)] * 4, me, own, others[m])
        for n, part in zip(range(4 * m, 4 * m + 4), parts):
            u, v = CLASSES[n]
            step = [-d for d in NEAREST[u, v]]
            pieces[u * 4 + v] = send(part, step + [0]) if any(step) else part
    return [pieces[kind] for kind in range(16)]


def lookup_kernel(me, addr, ends, *refs):
    z = place(me[0])[2]
    pieces, out, table, sums = refs[:16], refs[16], refs[17], refs[18:]
    for kind, piece in enumerate(pieces):

        def put(i, carry, piece=piece, kind=kind):
            at = pl.multiple_of((i & 3) * 128, 128)
            to = pl.multiple_of(kind * 2 * DEPTH + i * 128, 128)
            table[pl.ds(to, 128), :] = piece[i >> 2, pl.ds(at, 128), :]
            return carry

        lax.fori_loop(0, 8, put, 0)

    def step(i, carry):
        note = [(i * BLOCKS + j) * IDS for j in range(BLOCKS)]
        info = [n + z * 32 for n in note]
        first = [note[j] + ends[info[j]] for j in range(BLOCKS)]
        most = ends[info[0] + SAMP]
        for j in range(1, BLOCKS):
            most = jnp.maximum(most, ends[info[j] + SAMP])

        def chunk(k, totals):
            totals = list(totals)
            at = [f + k * CHUNK for f in first]
            to = k * CHUNK + 1
            for p in range(CHUNK):
                for j, prefix in enumerate(sums):
                    totals[j] = totals[j] + table[pl.ds(addr[at[j] + p], 1), :]
                    prefix[pl.ds(to + p, 1), :] = totals[j]
            return tuple(totals)

        lax.fori_loop(0, (most + CHUNK - 1) // CHUNK, chunk, (jnp.zeros((1, WIDTH), jnp.float32),) * BLOCKS)

        for j, prefix in enumerate(sums):
            row = (i * BLOCKS + j) * SAMP
            low = jnp.zeros((1, WIDTH), jnp.float32)
            for s in range(SAMP):
                upto = prefix[pl.ds(ends[info[j] + s + 1], 1), :]
                out[pl.ds(row + s, 1), :] = upto - low
                low = upto
        return carry

    for prefix in sums:
        prefix[0:1, :] = jnp.zeros((1, WIDTH), jnp.float32)
    lax.fori_loop(0, DEVICES // BLOCKS, step, 0)


def finish_kernel(order, parts, out):
    for col in range(TABLES):
        t = order[col]
        at = holders(t)
        out[:, col, :] = (parts[at[0]] + parts[at[1]]) + (parts[at[2]] + parts[at[3]])


def program(saved_rows, table_order, owner_shard, row_in_shard, bag_owner):
    me = lax.axis_index("d")
    scalars = me.reshape(1)
    lists = (owner_shard.reshape(TABLES, IDS), row_in_shard.reshape(TABLES, IDS), bag_owner.reshape(TABLES, IDS))
    pieces = restore(scalars, saved_rows.reshape(16, 2, DEPTH, WIDTH))
    (notes,) = pack(notes_kernel, [(DEVICES, 2)], scalars, *lists)
    notes = lax.all_to_all(notes, "d", split_axis=0, concat_axis=0, tiled=True)
    notes = notes.astype(jnp.int32)
    addr = jnp.pad(notes[:, 0].reshape(-1), (0, 2 * IDS))
    ends = notes[:, 1].reshape(-1)
    partial = pl.pallas_call(
        lookup_kernel,
        out_shape=jax.ShapeDtypeStruct((DEVICES * SAMP, WIDTH), jnp.float32),
        in_specs=[SCALARS] * 3 + in_vmem(16),
        out_specs=in_vmem(1)[0],
        scratch_shapes=[pltpu.VMEM((32 * DEPTH, WIDTH), jnp.float32)]
        + [pltpu.VMEM((IDS + 8, WIDTH), jnp.float32)] * BLOCKS,
        compiler_params=pltpu.CompilerParams(vmem_limit_bytes=12 << 20),
        name="lookup",
    )(scalars, addr, ends, *pieces)
    parts = lax.all_to_all(
        partial.reshape(DEVICES, SAMP, WIDTH), "d", split_axis=0, concat_axis=0, tiled=True
    )
    return pl.pallas_call(
        finish_kernel,
        out_shape=jax.ShapeDtypeStruct((SAMP, TABLES, WIDTH), jnp.float32),
        in_specs=[SCALARS] + in_vmem(1),
        out_specs=in_vmem(1)[0],
        name="finish",
    )(table_order, parts)


def solution(mesh):
    flat = Mesh(mesh.devices.reshape(DEVICES), ("d",))
    return jax.shard_map(
        program,
        mesh=flat,
        in_specs=(
            P(None, None, "d", None),
            P(),
            P(None, "d", None, None),
            P(None, "d", None),
            P(None, "d", None),
        ),
        out_specs=P("d", None, None),
        check_vma=False,
    )
```

```python
import functools

import jax
import jax.numpy as jnp
from jax import lax
from jax.experimental import pallas as pl
from jax.experimental.pallas import tpu as pltpu
from jax.sharding import Mesh, PartitionSpec as P


TABLES = 32
DEPTH = 512
WIDTH = 128
DEVICES = 128
IDS = 128
SAMP = 16
BLOCKS = 8
CHUNK = 8
NEAREST = {
    (2, 0): (2, 0, 0),
    (0, 2): (0, 2, 0),
    (2, 2): (0, 0, 2),
    (1, 0): (1, 0, 0),
    (3, 0): (-1, 0, 0),
    (0, 1): (0, 1, 0),
    (0, 3): (0, -1, 0),
    (1, 1): (0, 0, -1),
    (3, 3): (0, 0, 1),
    (1, 3): (1, -1, 0),
    (1, 2): (0, 1, -1),
    (2, 3): (-1, 0, 1),
    (3, 1): (-1, 1, 0),
    (3, 2): (0, -1, 1),
    (2, 1): (1, 0, -1),
    (0, 0): (0, 0, 0),
}
CLASSES = list(NEAREST)


def place(k):
    return (k >> 6) * 2 + ((k >> 1) & 1), (k >> 4) & 3, (k >> 2) & 3, k & 1


def device(x, y, z, c):
    return (x >> 1) * 64 + y * 16 + z * 4 + (x & 1) * 2 + c


def moved(step):
    pairs = []
    for k in range(DEVICES):
        at = [p + d for p, d in zip(place(k), step)]
        pairs.append((k, device(*[p & 3 for p in at[:3]], at[3] & 1)))
    return pairs


def holders(t):
    a, b, c = t >> 3, (t >> 1) & 3, t & 1
    return [device((a + z) & 3, (b + z) & 3, z, c) for z in range(4)]


def in_vmem(count):
    return [pl.BlockSpec(memory_space=pltpu.VMEM)] * count


SCALARS = pl.BlockSpec(memory_space=pltpu.SMEM)


def send(value, step):
    return lax.ppermute(value, "d", moved(step))


def half_kernel(theirs, classes, me, saved, *refs):
    outs, sems = refs[:-1], refs[-1]
    x, y, z, c = place(me[0])
    core = 1 - c if theirs else c
    copies = []
    for n, (u, v) in enumerate(classes):
        t = ((x - z - u) & 3) * 4 + ((y - z - v) & 3)
        copies.append(pltpu.make_async_copy(saved.at[t, core], outs[n // 4].at[n % 4], sems.at[n]))
        copies[-1].start()
    for copy in copies:
        copy.wait()


def pack_kernel(me, own, other, *outs):
    for n, out in enumerate(outs):
        out[0] = own[n]
        out[1] = other[n]


def notes_kernel(me, owner, row, bag, out):
    wanted = owner[...] * 1024 + row[...]
    depth = wanted >> 7
    sx, sy, sz, sc = place(wanted & 127)
    table = lax.broadcasted_iota(jnp.int32, (TABLES, IDS), 0)
    ta, tb, tc = table >> 3, (table >> 1) & 3, table & 1
    u, v = (sx - sz - ta) & 3, (sy - sz - tb) & 3
    kind = u * 4 + v
    holder = jnp.zeros((TABLES, IDS), jnp.int32)
    for (cu, cv), step in NEAREST.items():
        holder = jnp.where(kind == cu * 4 + cv, step[2], holder)
    holder = (sz - holder) & 3
    addr = (kind * 2 + (tc ^ sc)) * DEPTH + depth

    upper = lax.broadcasted_iota(jnp.int32, (IDS, IDS), 0) <= lax.broadcasted_iota(jnp.int32, (IDS, IDS), 1)
    upper = upper.astype(jnp.float32)
    is_in = [(holder == z).astype(jnp.float32) for z in range(4)]
    slot = jnp.zeros((TABLES, IDS), jnp.float32)
    offset = jnp.zeros((TABLES, 1), jnp.float32)
    for z in range(4):
        rank = jnp.dot(is_in[z], upper, preferred_element_type=jnp.float32)
        slot = slot + is_in[z] * (rank + (offset - 1.0))
        offset = offset + jnp.sum(is_in[z], axis=1, keepdims=True)
    slots = jnp.transpose(slot)
    bags = jnp.transpose(bag[...].astype(jnp.float32))
    high, low = (addr >> 8).astype(jnp.float32), (addr & 255).astype(jnp.float32)

    lane = lax.broadcasted_iota(jnp.int32, (IDS, IDS), 1)
    lanes = lane.astype(jnp.float32)
    bound = jnp.where((lane & 31) == 0, SAMP, (lane & 31) - 1).astype(jnp.float32)
    kind = lax.broadcasted_iota(jnp.int32, (8, IDS), 0) - 2
    at = lax.broadcasted_iota(jnp.int32, (8, IDS), 1)
    before = ((at & 31) == 0) & (kind < (at >> 5)) & (kind >= 0)
    counted = (before | (((at & 31) != 0) & (kind == (at >> 5)))).astype(jnp.float32)
    for t in range(TABLES):
        rows = [high[t : t + 1], low[t : t + 1]] + [m[t : t + 1] for m in is_in]
        rows = jnp.concatenate(rows + [jnp.zeros((2, IDS), jnp.float32)], axis=0)
        chosen = (slots[:, t : t + 1] == lanes).astype(jnp.float32)
        within = (bags[:, t : t + 1] <= bound).astype(jnp.float32)
        got = jnp.dot(rows, chosen, preferred_element_type=jnp.float32)
        ends = jnp.dot(rows, within, preferred_element_type=jnp.float32)
        got = got[0:1] * 256.0 + got[1:2]
        ends = jnp.sum(ends * counted, axis=0, keepdims=True)
        for k in holders(t):
            out[k, 0:1, :] = got
            out[k, 1:2, :] = ends


def pack(kernel, shapes, me, *args):
    return list(pl.pallas_call(
        kernel,
        out_shape=[jax.ShapeDtypeStruct(shape + (WIDTH,), jnp.float32) for shape in shapes],
        in_specs=[SCALARS] + in_vmem(len(args)),
        out_specs=in_vmem(len(shapes)),
        compiler_params=pltpu.CompilerParams(vmem_limit_bytes=6 << 20),
    )(me, *args))


def halves(theirs, classes, me, saved):
    return list(pl.pallas_call(
        functools.partial(half_kernel, theirs, classes),
        out_shape=[jax.ShapeDtypeStruct((4, DEPTH, WIDTH), jnp.float32)] * (len(classes) // 4),
        in_specs=[SCALARS, pl.BlockSpec(memory_space=pltpu.HBM)],
        out_specs=in_vmem(len(classes) // 4),
        scratch_shapes=[pltpu.SemaphoreType.DMA((len(classes),))],
        compiler_params=pltpu.CompilerParams(vmem_limit_bytes=46 << 20),
    )(me, saved))


def restore(me, saved):
    theirs = halves(True, CLASSES[:4], me, saved)
    own = halves(False, CLASSES, me, saved)
    theirs += halves(True, CLASSES[4:], me, saved)
    others = [send(theirs[m], (0, 0, 0, 1)) for m in range(4)]
    pieces = {}
    for m in range(4):
        parts = pack(pack_kernel, [(2, DEPTH)] * 4, me, own[m], others[m])
        for n, part in zip(range(4 * m, 4 * m + 4), parts):
            u, v = CLASSES[n]
            step = [-d for d in NEAREST[u, v]]
            pieces[u * 4 + v] = send(part, step + [0]) if any(step) else part
    return [pieces[kind] for kind in range(16)]


def lookup_kernel(me, addr, ends, *refs):
    z = place(me[0])[2]
    pieces, out, table, sums = refs[:16], refs[16], refs[17], refs[18:]
    for kind, piece in enumerate(pieces):

        def put(i, carry, piece=piece, kind=kind):
            at = pl.multiple_of((i & 3) * 128, 128)
            to = pl.multiple_of(kind * 2 * DEPTH + i * 128, 128)
            table[pl.ds(to, 128), :] = piece[i >> 2, pl.ds(at, 128), :]
            return carry

        lax.fori_loop(0, 8, put, 0)

    def step(i, carry):
        note = [(i * BLOCKS + j) * IDS for j in range(BLOCKS)]
        info = [n + z * 32 for n in note]
        first = [note[j] + ends[info[j]] for j in range(BLOCKS)]
        most = ends[info[0] + SAMP]
        for j in range(1, BLOCKS):
            most = jnp.maximum(most, ends[info[j] + SAMP])

        def chunk(k, totals):
            totals = list(totals)
            at = [addr.at[pl.ds(f + k * CHUNK, CHUNK)] for f in first]
            to = k * CHUNK + 1
            for p in range(CHUNK):
                for j, prefix in enumerate(sums):
                    totals[j] = totals[j] + table[pl.ds(at[j][p], 1), :]
                    prefix[pl.ds(to + p, 1), :] = totals[j]
            return tuple(totals)

        lax.fori_loop(0, (most + CHUNK - 1) // CHUNK, chunk, (jnp.zeros((1, WIDTH), jnp.float32),) * BLOCKS)

        for j, prefix in enumerate(sums):
            row = (i * BLOCKS + j) * SAMP
            low = jnp.zeros((1, WIDTH), jnp.float32)
            bags = ends.at[pl.ds(info[j], 32)]
            for s in range(SAMP):
                upto = prefix[pl.ds(bags[s + 1], 1), :]
                out[pl.ds(row + s, 1), :] = upto - low
                low = upto
        return carry

    for prefix in sums:
        prefix[0:1, :] = jnp.zeros((1, WIDTH), jnp.float32)
    lax.fori_loop(0, DEVICES // BLOCKS, step, 0)


def finish_kernel(order, parts, out):
    for col in range(TABLES):
        t = order[col]
        at = holders(t)
        out[:, col, :] = (parts[at[0]] + parts[at[1]]) + (parts[at[2]] + parts[at[3]])


def program(saved_rows, table_order, owner_shard, row_in_shard, bag_owner):
    me = lax.axis_index("d")
    scalars = me.reshape(1)
    lists = (owner_shard.reshape(TABLES, IDS), row_in_shard.reshape(TABLES, IDS), bag_owner.reshape(TABLES, IDS))
    pieces = restore(scalars, saved_rows.reshape(16, 2, DEPTH, WIDTH))
    (notes,) = pack(notes_kernel, [(DEVICES, 2)], scalars, *lists)
    notes = lax.all_to_all(notes, "d", split_axis=0, concat_axis=0, tiled=True)
    notes = notes.astype(jnp.int32)
    addr = jnp.pad(notes[:, 0].reshape(-1), (0, 2 * IDS))
    ends = notes[:, 1].reshape(-1)
    partial = pl.pallas_call(
        lookup_kernel,
        out_shape=jax.ShapeDtypeStruct((DEVICES * SAMP, WIDTH), jnp.float32),
        in_specs=[SCALARS] * 3 + in_vmem(16),
        out_specs=in_vmem(1)[0],
        scratch_shapes=[pltpu.VMEM((32 * DEPTH, WIDTH), jnp.float32)]
        + [pltpu.VMEM((IDS + 8, WIDTH), jnp.float32)] * BLOCKS,
        compiler_params=pltpu.CompilerParams(vmem_limit_bytes=12 << 20),
        name="lookup",
    )(scalars, addr, ends, *pieces)
    parts = lax.all_to_all(
        partial.reshape(DEVICES, SAMP, WIDTH), "d", split_axis=0, concat_axis=0, tiled=True
    )
    return pl.pallas_call(
        finish_kernel,
        out_shape=jax.ShapeDtypeStruct((SAMP, TABLES, WIDTH), jnp.float32),
        in_specs=[SCALARS] + in_vmem(1),
        out_specs=in_vmem(1)[0],
        compiler_params=pltpu.CompilerParams(vmem_limit_bytes=4 << 20),
        name="finish",
    )(table_order, parts)


def solution(mesh):
    flat = Mesh(mesh.devices.reshape(DEVICES), ("d",))
    return jax.shard_map(
        program,
        mesh=flat,
        in_specs=(
            P(None, None, "d", None),
            P(),
            P(None, "d", None, None),
            P(None, "d", None),
            P(None, "d", None),
        ),
        out_specs=P("d", None, None),
        check_vma=False,
    )
```

```python
import functools

import jax
import jax.numpy as jnp
from jax import lax
from jax.experimental import pallas as pl
from jax.experimental.pallas import tpu as pltpu
from jax.sharding import Mesh, PartitionSpec as P


TABLES = 32
DEPTH = 512
WIDTH = 128
DEVICES = 128
IDS = 128
SAMP = 16
BLOCKS = 8
CHUNK = 8
NEAREST = {
    (3, 0): (-1, 0, 0),
    (3, 1): (-1, 1, 0),
    (1, 0): (1, 0, 0),
    (1, 3): (1, -1, 0),
    (0, 3): (0, -1, 0),
    (3, 2): (0, -1, 1),
    (0, 1): (0, 1, 0),
    (1, 2): (0, 1, -1),
    (1, 1): (0, 0, -1),
    (2, 1): (1, 0, -1),
    (3, 3): (0, 0, 1),
    (2, 3): (-1, 0, 1),
    (2, 0): (2, 0, 0),
    (0, 2): (0, 2, 0),
    (2, 2): (0, 0, 2),
    (0, 0): (0, 0, 0),
}
CLASSES = list(NEAREST)
HOPS = [tuple(-d for d in NEAREST[CLASSES[2 * n]]) for n in range(6)]
TURNS = [
    tuple(-d - h for d, h in zip(NEAREST[CLASSES[2 * n + 1]], HOPS[n])) for n in range(6)
]


def place(k):
    return (k >> 6) * 2 + ((k >> 1) & 1), (k >> 4) & 3, (k >> 2) & 3, k & 1


def device(x, y, z, c):
    return (x >> 1) * 64 + y * 16 + z * 4 + (x & 1) * 2 + c


def moved(step):
    pairs = []
    for k in range(DEVICES):
        at = [p + d for p, d in zip(place(k), step)]
        pairs.append((k, device(*[p & 3 for p in at[:3]], at[3] & 1)))
    return pairs


def holders(t):
    a, b, c = t >> 3, (t >> 1) & 3, t & 1
    return [device((a + z) & 3, (b + z) & 3, z, c) for z in range(4)]


def in_vmem(count):
    return [pl.BlockSpec(memory_space=pltpu.VMEM)] * count


SCALARS = pl.BlockSpec(memory_space=pltpu.SMEM)


def send(value, step):
    return lax.ppermute(value, "d", moved(step))


def half_kernel(theirs, classes, me, saved, *refs):
    outs, sems = refs[:-1], refs[-1]
    x, y, z, c = place(me[0])
    core = 1 - c if theirs else c
    copies = []
    for n, (u, v) in enumerate(classes):
        t = ((x - z - u) & 3) * 4 + ((y - z - v) & 3)
        copies.append(pltpu.make_async_copy(saved.at[t, core], outs[n // 4].at[n % 4], sems.at[n]))
        copies[-1].start()
    for copy in copies:
        copy.wait()


def pack_kernel(me, own, other, *outs):
    per_out = 4 // len(outs)
    for n in range(4):
        outs[n // per_out][n % per_out * 2] = own[n]
        outs[n // per_out][n % per_out * 2 + 1] = other[n]


def onward_kernel(me, got, out):
    out[...] = got[2:]


def notes_kernel(me, owner, row, bag, out):
    wanted = owner[...] * 1024 + row[...]
    depth = wanted >> 7
    sx, sy, sz, sc = place(wanted & 127)
    table = lax.broadcasted_iota(jnp.int32, (TABLES, IDS), 0)
    ta, tb, tc = table >> 3, (table >> 1) & 3, table & 1
    u, v = (sx - sz - ta) & 3, (sy - sz - tb) & 3
    kind = u * 4 + v
    holder = jnp.zeros((TABLES, IDS), jnp.int32)
    for (cu, cv), step in NEAREST.items():
        holder = jnp.where(kind == cu * 4 + cv, step[2], holder)
    holder = (sz - holder) & 3
    addr = (kind * 2 + (tc ^ sc)) * DEPTH + depth

    upper = lax.broadcasted_iota(jnp.int32, (IDS, IDS), 0) <= lax.broadcasted_iota(jnp.int32, (IDS, IDS), 1)
    upper = upper.astype(jnp.float32)
    is_in = [(holder == z).astype(jnp.float32) for z in range(4)]
    slot = jnp.zeros((TABLES, IDS), jnp.float32)
    offset = jnp.zeros((TABLES, 1), jnp.float32)
    for z in range(4):
        rank = jnp.dot(is_in[z], upper, preferred_element_type=jnp.float32)
        slot = slot + is_in[z] * (rank + (offset - 1.0))
        offset = offset + jnp.sum(is_in[z], axis=1, keepdims=True)
    slots = jnp.transpose(slot)
    bags = jnp.transpose(bag[...].astype(jnp.float32))
    high, low = (addr >> 8).astype(jnp.float32), (addr & 255).astype(jnp.float32)

    lane = lax.broadcasted_iota(jnp.int32, (IDS, IDS), 1)
    lanes = lane.astype(jnp.float32)
    bound = jnp.where((lane & 31) == 0, SAMP, (lane & 31) - 1).astype(jnp.float32)
    kind = lax.broadcasted_iota(jnp.int32, (8, IDS), 0) - 2
    at = lax.broadcasted_iota(jnp.int32, (8, IDS), 1)
    before = ((at & 31) == 0) & (kind < (at >> 5)) & (kind >= 0)
    counted = (before | (((at & 31) != 0) & (kind == (at >> 5)))).astype(jnp.float32)
    for t in range(TABLES):
        rows = [high[t : t + 1], low[t : t + 1]] + [m[t : t + 1] for m in is_in]
        rows = jnp.concatenate(rows + [jnp.zeros((2, IDS), jnp.float32)], axis=0)
        chosen = (slots[:, t : t + 1] == lanes).astype(jnp.float32)
        within = (bags[:, t : t + 1] <= bound).astype(jnp.float32)
        got = jnp.dot(rows, chosen, preferred_element_type=jnp.float32)
        ends = jnp.dot(rows, within, preferred_element_type=jnp.float32)
        got = got[0:1] * 256.0 + got[1:2]
        ends = jnp.sum(ends * counted, axis=0, keepdims=True)
        for k in holders(t):
            out[k, 0:1, :] = got
            out[k, 1:2, :] = ends


def pack(kernel, shapes, me, *args):
    return list(pl.pallas_call(
        kernel,
        out_shape=[jax.ShapeDtypeStruct(shape + (WIDTH,), jnp.float32) for shape in shapes],
        in_specs=[SCALARS] + in_vmem(len(args)),
        out_specs=in_vmem(len(shapes)),
        compiler_params=pltpu.CompilerParams(vmem_limit_bytes=6 << 20),
    )(me, *args))


def halves(theirs, classes, me, saved):
    return list(pl.pallas_call(
        functools.partial(half_kernel, theirs, classes),
        out_shape=[jax.ShapeDtypeStruct((4, DEPTH, WIDTH), jnp.float32)] * (len(classes) // 4),
        in_specs=[SCALARS, pl.BlockSpec(memory_space=pltpu.HBM)],
        out_specs=in_vmem(len(classes) // 4),
        scratch_shapes=[pltpu.SemaphoreType.DMA((len(classes),))],
        compiler_params=pltpu.CompilerParams(vmem_limit_bytes=46 << 20),
    )(me, saved))


def restore(me, saved):
    theirs = halves(True, CLASSES[:4], me, saved)
    own = halves(False, CLASSES, me, saved)
    theirs += halves(True, CLASSES[4:], me, saved)
    others = [send(theirs[m], (0, 0, 0, 1)) for m in range(4)]
    pieces, turning = {}, []
    for m in range(3):
        parts = pack(pack_kernel, [(4, DEPTH)] * 2, me, own[m], others[m])
        for n, part in zip((2 * m, 2 * m + 1), parts):
            got = send(part, HOPS[n] + (0,))
            pieces[CLASSES[2 * n]] = got
            turning.append(got)
    parts = pack(pack_kernel, [(2, DEPTH)] * 4, me, own[3], others[3])
    for n, part in enumerate(parts):
        step = NEAREST[CLASSES[12 + n]]
        pieces[CLASSES[12 + n]] = send(part, step + (0,)) if any(step) else part
    for n, got in enumerate(turning):
        (part,) = pack(onward_kernel, [(2, DEPTH)], me, got)
        pieces[CLASSES[2 * n + 1]] = send(part, TURNS[n] + (0,))
    return [pieces[kind >> 2, kind & 3] for kind in range(16)]


def lookup_kernel(me, places, bounds, *refs):
    z = place(me[0])[2]
    pieces, out, table, addr, ends, sems, sums = refs[:16], *refs[16:21], refs[21:]
    fetches = [
        pltpu.make_async_copy(places, addr, sems.at[0]),
        pltpu.make_async_copy(bounds, ends, sems.at[1]),
    ]
    for fetch in fetches:
        fetch.start()
    for kind, piece in enumerate(pieces):

        def put(i, carry, piece=piece, kind=kind):
            at = pl.multiple_of((i & 3) * 128, 128)
            to = pl.multiple_of(kind * 2 * DEPTH + i * 128, 128)
            table[pl.ds(to, 128), :] = piece[i >> 2, pl.ds(at, 128), :]
            return carry

        lax.fori_loop(0, 8, put, 0)
    for fetch in fetches:
        fetch.wait()

    def step(i, carry):
        note = [(i * BLOCKS + j) * IDS for j in range(BLOCKS)]
        info = [n + z * 32 for n in note]
        first = [note[j] + ends[info[j]] for j in range(BLOCKS)]
        most = ends[info[0] + SAMP]
        for j in range(1, BLOCKS):
            most = jnp.maximum(most, ends[info[j] + SAMP])

        def chunk(k, totals):
            totals = list(totals)
            at = [addr.at[pl.ds(f + k * CHUNK, CHUNK)] for f in first]
            to = k * CHUNK + 1
            for p in range(CHUNK):
                for j, prefix in enumerate(sums):
                    totals[j] = totals[j] + table[pl.ds(at[j][p], 1), :]
                    prefix[pl.ds(to + p, 1), :] = totals[j]
            return tuple(totals)

        lax.fori_loop(0, (most + CHUNK - 1) // CHUNK, chunk, (jnp.zeros((1, WIDTH), jnp.float32),) * BLOCKS)

        for j, prefix in enumerate(sums):
            row = (i * BLOCKS + j) * SAMP
            low = jnp.zeros((1, WIDTH), jnp.float32)
            bags = ends.at[pl.ds(info[j], 32)]
            for s in range(SAMP):
                upto = prefix[pl.ds(bags[s + 1], 1), :]
                out[pl.ds(row + s, 1), :] = upto - low
                low = upto
        return carry

    for prefix in sums:
        prefix[0:1, :] = jnp.zeros((1, WIDTH), jnp.float32)
    lax.fori_loop(0, DEVICES // BLOCKS, step, 0)


def finish_kernel(order, parts, out):
    for col in range(TABLES):
        t = order[col]
        at = holders(t)
        out[:, col, :] = (parts[at[0]] + parts[at[1]]) + (parts[at[2]] + parts[at[3]])


def program(saved_rows, table_order, owner_shard, row_in_shard, bag_owner):
    me = lax.axis_index("d")
    scalars = me.reshape(1)
    lists = (owner_shard.reshape(TABLES, IDS), row_in_shard.reshape(TABLES, IDS), bag_owner.reshape(TABLES, IDS))
    pieces = restore(scalars, saved_rows.reshape(16, 2, DEPTH, WIDTH))
    (notes,) = pack(notes_kernel, [(DEVICES, 2)], scalars, *lists)
    notes = lax.all_to_all(notes, "d", split_axis=0, concat_axis=0, tiled=True)
    notes = notes.astype(jnp.int32)
    addr = jnp.pad(notes[:, 0].reshape(-1), (0, 2 * IDS))
    ends = notes[:, 1].reshape(-1)
    partial = pl.pallas_call(
        lookup_kernel,
        out_shape=jax.ShapeDtypeStruct((DEVICES * SAMP, WIDTH), jnp.float32),
        in_specs=[SCALARS] + in_vmem(18),
        out_specs=in_vmem(1)[0],
        scratch_shapes=[
            pltpu.VMEM((32 * DEPTH, WIDTH), jnp.float32),
            pltpu.SMEM((DEVICES * IDS + 2 * IDS,), jnp.int32),
            pltpu.SMEM((DEVICES * IDS,), jnp.int32),
            pltpu.SemaphoreType.DMA((2,)),
        ]
        + [pltpu.VMEM((IDS + 8, WIDTH), jnp.float32)] * BLOCKS,
        compiler_params=pltpu.CompilerParams(vmem_limit_bytes=12 << 20),
        name="lookup",
    )(scalars, addr, ends, *pieces)
    parts = lax.all_to_all(
        partial.reshape(DEVICES, SAMP, WIDTH), "d", split_axis=0, concat_axis=0, tiled=True
    )
    return pl.pallas_call(
        finish_kernel,
        out_shape=jax.ShapeDtypeStruct((SAMP, TABLES, WIDTH), jnp.float32),
        in_specs=[SCALARS] + in_vmem(1),
        out_specs=in_vmem(1)[0],
        compiler_params=pltpu.CompilerParams(vmem_limit_bytes=4 << 20),
        name="finish",
    )(table_order, parts)


def solution(mesh):
    flat = Mesh(mesh.devices.reshape(DEVICES), ("d",))
    return jax.shard_map(
        program,
        mesh=flat,
        in_specs=(
            P(None, None, "d", None),
            P(),
            P(None, "d", None, None),
            P(None, "d", None),
            P(None, "d", None),
        ),
        out_specs=P("d", None, None),
        check_vma=False,
    )
```

```python
import functools

import jax
import jax.numpy as jnp
from jax import lax
from jax.experimental import pallas as pl
from jax.experimental.pallas import tpu as pltpu
from jax.sharding import Mesh, PartitionSpec as P


TABLES = 32
DEPTH = 512
WIDTH = 128
DEVICES = 128
IDS = 128
SAMP = 16
BLOCKS = 8
CHUNK = 8
NEAREST = {
    (2, 0): (2, 0, 0),
    (0, 2): (0, 2, 0),
    (2, 2): (0, 0, 2),
    (3, 1): (-1, 1, 0),
    (1, 3): (1, -1, 0),
    (1, 1): (0, 0, -1),
    (3, 3): (0, 0, 1),
    (2, 1): (1, 0, -1),
    (2, 3): (-1, 0, 1),
    (0, 1): (0, 1, 0),
    (0, 3): (0, -1, 0),
    (3, 2): (0, -1, 1),
    (1, 2): (0, 1, -1),
    (1, 0): (1, 0, 0),
    (3, 0): (-1, 0, 0),
    (0, 0): (0, 0, 0),
}
CLASSES = list(NEAREST)


def place(k):
    return (k >> 6) * 2 + ((k >> 1) & 1), (k >> 4) & 3, (k >> 2) & 3, k & 1


def device(x, y, z, c):
    return (x >> 1) * 64 + y * 16 + z * 4 + (x & 1) * 2 + c


def moved(step):
    pairs = []
    for k in range(DEVICES):
        at = [p + d for p, d in zip(place(k), step)]
        pairs.append((k, device(*[p & 3 for p in at[:3]], at[3] & 1)))
    return pairs


def holders(t):
    a, b, c = t >> 3, (t >> 1) & 3, t & 1
    return [device((a + z) & 3, (b + z) & 3, z, c) for z in range(4)]


def in_vmem(count):
    return [pl.BlockSpec(memory_space=pltpu.VMEM)] * count


SCALARS = pl.BlockSpec(memory_space=pltpu.SMEM)


def send(value, step):
    return lax.ppermute(value, "d", moved(step))


def half_kernel(theirs, classes, me, saved, *refs):
    outs, sems = refs[:-1], refs[-1]
    x, y, z, c = place(me[0])
    core = 1 - c if theirs else c
    copies = []
    for n, (u, v) in enumerate(classes):
        t = ((x - z - u) & 3) * 4 + ((y - z - v) & 3)
        copies.append(pltpu.make_async_copy(saved.at[t, core], outs[n // 4].at[n % 4], sems.at[n]))
        copies[-1].start()
    for copy in copies:
        copy.wait()


def pack_kernel(me, own, other, *outs):
    for n, out in enumerate(outs):
        out[0] = own[n]
        out[1] = other[n]


def notes_kernel(me, owner, row, bag, out):
    wanted = owner[...] * 1024 + row[...]
    depth = wanted >> 7
    sx, sy, sz, sc = place(wanted & 127)
    table = lax.broadcasted_iota(jnp.int32, (TABLES, IDS), 0)
    ta, tb, tc = table >> 3, (table >> 1) & 3, table & 1
    u, v = (sx - sz - ta) & 3, (sy - sz - tb) & 3
    kind = u * 4 + v
    holder = jnp.zeros((TABLES, IDS), jnp.int32)
    for (cu, cv), step in NEAREST.items():
        holder = jnp.where(kind == cu * 4 + cv, step[2], holder)
    holder = (sz - holder) & 3
    addr = (kind * 2 + (tc ^ sc)) * DEPTH + depth

    upper = lax.broadcasted_iota(jnp.int32, (IDS, IDS), 0) <= lax.broadcasted_iota(jnp.int32, (IDS, IDS), 1)
    upper = upper.astype(jnp.float32)
    is_in = [(holder == z).astype(jnp.float32) for z in range(4)]
    slot = jnp.zeros((TABLES, IDS), jnp.float32)
    offset = jnp.zeros((TABLES, 1), jnp.float32)
    for z in range(4):
        rank = jnp.dot(is_in[z], upper, preferred_element_type=jnp.float32)
        slot = slot + is_in[z] * (rank + (offset - 1.0))
        offset = offset + jnp.sum(is_in[z], axis=1, keepdims=True)
    slots = jnp.transpose(slot)
    bags = jnp.transpose(bag[...].astype(jnp.float32))
    high, low = (addr >> 8).astype(jnp.float32), (addr & 255).astype(jnp.float32)

    lane = lax.broadcasted_iota(jnp.int32, (IDS, IDS), 1)
    lanes = lane.astype(jnp.float32)
    bound = jnp.where((lane & 31) == 0, SAMP, (lane & 31) - 1).astype(jnp.float32)
    kind = lax.broadcasted_iota(jnp.int32, (8, IDS), 0) - 2
    at = lax.broadcasted_iota(jnp.int32, (8, IDS), 1)
    before = ((at & 31) == 0) & (kind < (at >> 5)) & (kind >= 0)
    counted = (before | (((at & 31) != 0) & (kind == (at >> 5)))).astype(jnp.float32)
    for t in range(TABLES):
        rows = [high[t : t + 1], low[t : t + 1]] + [m[t : t + 1] for m in is_in]
        rows = jnp.concatenate(rows + [jnp.zeros((2, IDS), jnp.float32)], axis=0)
        chosen = (slots[:, t : t + 1] == lanes).astype(jnp.float32)
        within = (bags[:, t : t + 1] <= bound).astype(jnp.float32)
        got = jnp.dot(rows, chosen, preferred_element_type=jnp.float32)
        ends = jnp.dot(rows, within, preferred_element_type=jnp.float32)
        got = got[0:1] * 256.0 + got[1:2]
        ends = jnp.sum(ends * counted, axis=0, keepdims=True)
        for k in holders(t):
            out[k, 0:1, :] = got
            out[k, 1:2, :] = ends


def pack(kernel, shapes, me, *args):
    return list(pl.pallas_call(
        kernel,
        out_shape=[jax.ShapeDtypeStruct(shape + (WIDTH,), jnp.float32) for shape in shapes],
        in_specs=[SCALARS] + in_vmem(len(args)),
        out_specs=in_vmem(len(shapes)),
        compiler_params=pltpu.CompilerParams(vmem_limit_bytes=6 << 20),
    )(me, *args))


def halves(theirs, classes, me, saved):
    return list(pl.pallas_call(
        functools.partial(half_kernel, theirs, classes),
        out_shape=[jax.ShapeDtypeStruct((4, DEPTH, WIDTH), jnp.float32)] * (len(classes) // 4),
        in_specs=[SCALARS, pl.BlockSpec(memory_space=pltpu.HBM)],
        out_specs=in_vmem(len(classes) // 4),
        scratch_shapes=[pltpu.SemaphoreType.DMA((len(classes),))],
        compiler_params=pltpu.CompilerParams(vmem_limit_bytes=46 << 20),
    )(me, saved))


def restore(me, saved):
    theirs = halves(True, CLASSES[:4], me, saved)
    own = halves(False, CLASSES, me, saved)
    theirs += halves(True, CLASSES[4:], me, saved)
    others = [send(theirs[m], (0, 0, 0, 1)) for m in range(4)]
    pieces = {}
    for m in range(4):
        parts = pack(pack_kernel, [(2, DEPTH)] * 4, me, own[m], others[m])
        for n, part in zip(range(4 * m, 4 * m + 4), parts):
            u, v = CLASSES[n]
            step = [-d for d in NEAREST[u, v]]
            pieces[u * 4 + v] = send(part, step + [0]) if any(step) else part
    return [pieces[kind] for kind in range(16)]


def lookup_kernel(me, places, bounds, *refs):
    z = place(me[0])[2]
    pieces, out, table, addr, ends, sems, sums = refs[:16], *refs[16:21], refs[21:]
    fetches = [
        pltpu.make_async_copy(places, addr, sems.at[0]),
        pltpu.make_async_copy(bounds, ends, sems.at[1]),
    ]
    for fetch in fetches:
        fetch.start()
    for kind, piece in enumerate(pieces):

        def put(i, carry, piece=piece, kind=kind):
            at = pl.multiple_of((i & 3) * 128, 128)
            to = pl.multiple_of(kind * 2 * DEPTH + i * 128, 128)
            table[pl.ds(to, 128), :] = piece[i >> 2, pl.ds(at, 128), :]
            return carry

        lax.fori_loop(0, 8, put, 0)
    for fetch in fetches:
        fetch.wait()

    def step(i, carry):
        note = [(i * BLOCKS + j) * IDS for j in range(BLOCKS)]
        info = [n + z * 32 for n in note]
        first = [note[j] + ends[info[j]] for j in range(BLOCKS)]
        most = ends[info[0] + SAMP]
        for j in range(1, BLOCKS):
            most = jnp.maximum(most, ends[info[j] + SAMP])

        def chunk(k, totals):
            totals = list(totals)
            at = [addr.at[pl.ds(f + k * CHUNK, CHUNK)] for f in first]
            to = k * CHUNK + 1
            for p in range(CHUNK):
                for j, prefix in enumerate(sums):
                    totals[j] = totals[j] + table[pl.ds(at[j][p], 1), :]
                    prefix[pl.ds(to + p, 1), :] = totals[j]
            return tuple(totals)

        lax.fori_loop(0, (most + CHUNK - 1) // CHUNK, chunk, (jnp.zeros((1, WIDTH), jnp.float32),) * BLOCKS)

        for j, prefix in enumerate(sums):
            row = (i * BLOCKS + j) * SAMP
            low = jnp.zeros((1, WIDTH), jnp.float32)
            bags = ends.at[pl.ds(info[j], 32)]
            for s in range(SAMP):
                upto = prefix[pl.ds(bags[s + 1], 1), :]
                out[pl.ds(row + s, 1), :] = upto - low
                low = upto
        return carry

    for prefix in sums:
        prefix[0:1, :] = jnp.zeros((1, WIDTH), jnp.float32)
    lax.fori_loop(0, DEVICES // BLOCKS, step, 0)


def finish_kernel(order, parts, out):
    for col in range(TABLES):
        t = order[col]
        at = holders(t)
        out[:, col, :] = (parts[at[0]] + parts[at[1]]) + (parts[at[2]] + parts[at[3]])


def program(saved_rows, table_order, owner_shard, row_in_shard, bag_owner):
    me = lax.axis_index("d")
    scalars = me.reshape(1)
    lists = (owner_shard.reshape(TABLES, IDS), row_in_shard.reshape(TABLES, IDS), bag_owner.reshape(TABLES, IDS))
    pieces = restore(scalars, saved_rows.reshape(16, 2, DEPTH, WIDTH))
    (notes,) = pack(notes_kernel, [(DEVICES, 2)], scalars, *lists)
    notes = lax.all_to_all(notes, "d", split_axis=0, concat_axis=0, tiled=True)
    notes = notes.astype(jnp.int32)
    addr = jnp.pad(notes[:, 0].reshape(-1), (0, 2 * IDS))
    ends = notes[:, 1].reshape(-1)
    partial = pl.pallas_call(
        lookup_kernel,
        out_shape=jax.ShapeDtypeStruct((DEVICES * SAMP, WIDTH), jnp.float32),
        in_specs=[SCALARS] + in_vmem(18),
        out_specs=in_vmem(1)[0],
        scratch_shapes=[
            pltpu.VMEM((32 * DEPTH, WIDTH), jnp.float32),
            pltpu.SMEM((DEVICES * IDS + 2 * IDS,), jnp.int32),
            pltpu.SMEM((DEVICES * IDS,), jnp.int32),
            pltpu.SemaphoreType.DMA((2,)),
        ]
        + [pltpu.VMEM((IDS + 8, WIDTH), jnp.float32)] * BLOCKS,
        compiler_params=pltpu.CompilerParams(vmem_limit_bytes=12 << 20),
        name="lookup",
    )(scalars, addr, ends, *pieces)
    parts = lax.all_to_all(
        partial.reshape(DEVICES, SAMP, WIDTH), "d", split_axis=0, concat_axis=0, tiled=True
    )
    return pl.pallas_call(
        finish_kernel,
        out_shape=jax.ShapeDtypeStruct((SAMP, TABLES, WIDTH), jnp.float32),
        in_specs=[SCALARS] + in_vmem(1),
        out_specs=in_vmem(1)[0],
        compiler_params=pltpu.CompilerParams(vmem_limit_bytes=4 << 20),
        name="finish",
    )(table_order, parts)


def solution(mesh):
    flat = Mesh(mesh.devices.reshape(DEVICES), ("d",))
    return jax.shard_map(
        program,
        mesh=flat,
        in_specs=(
            P(None, None, "d", None),
            P(),
            P(None, "d", None, None),
            P(None, "d", None),
            P(None, "d", None),
        ),
        out_specs=P("d", None, None),
        check_vma=False,
    )
```
